32 devices in a mesh: band: 16 (over z, y, core), chan: 2 (over x).
Axes of the slice: x: 2, y: 2, z: 4, core: 2. Of those that a mesh axis runs over, the one named last changes fastest.
Arguments:
- fine_features: bfloat16 [2, 192, 128, 512], P(None, 'chan', 'band'), may hold values from -100 to 100
- coarse_level: bfloat16 [2, 256, 64, 256], P(None, 'chan', 'band'), may hold values from -100 to 100
- lat_weight: bfloat16 [256, 192], P('chan'), may hold values from -0.4375 to 0.4375
- lat_gain: bfloat16 [256], P('chan'), may hold values from 0.099609375 to 1.8984375
- lat_shift: bfloat16 [256], P('chan'), may hold values from -3 to 3
- out_weight: bfloat16 [3, 3, 256, 256], P(None, None, 'chan'), may hold values from -0.125 to 0.125
- out_gain: bfloat16 [256], P('chan'), may hold values from 0.099609375 to 1.8984375
- out_shift: bfloat16 [256], P('chan'), may hold values from -3 to 3
- mask_weight: bfloat16 [256, 256], P('chan'), may hold values from -0.375 to 0.375
- mask_bias: bfloat16 [256], P('chan'), may hold values from -1.796875 to 1.796875
- queries: bfloat16 [200, 256], replicated, may hold values from -128 to 128
Outputs:
- log_probs: float32 [2, 200, 128, 512], P(None, None, ('band', 'chan'))
The draws below stay inside these ranges and needn't reach their ends.
All inputs are finite; a program needn't handle non-finite values.
Results may differ from the reference program's by a relative error of at most 0.0058.
Values may be sent and summed in bfloat16 or wider, within the bound.
A program may use at most 128 MiB of HBM per device.

```python
import jax
import jax.numpy as jnp
from jax import lax

D = 256
C4 = 192
QUERIES = 200
GROUPS = 32
IMAGES = 2
COLS = 512
H4 = 128


def banded_field(key, images, channels, height, width):
    key_noise = jax.random.fold_in(key, 0)
    key_rows = jax.random.fold_in(key, 1)
    key_cols = jax.random.fold_in(key, 2)
    key_offset = jax.random.fold_in(key, 4)
    positions = jnp.arange(height, dtype=jnp.float32) / max(height - 1, 1)
    ramp = 3.0 ** positions
    row_scale = ramp[None, :] * jnp.exp(jax.random.uniform(key_rows, (images, height), jnp.float32, -0.8, 0.8))
    col_scale = jnp.exp(jax.random.uniform(key_cols, (images, width), jnp.float32, -0.8, 0.8))
    scale = row_scale[:, None, :, None] * col_scale[:, None, None, :]
    offset = jax.random.uniform(key_offset, (images, channels, 1, 1), jnp.float32, -3.0, 3.0)
    noise = jax.random.truncated_normal(key_noise, -4.0, 4.0, (images, channels, height, width), jnp.float32)
    values = noise * scale + offset * ramp[None, None, :, None]
    return values


def draw_fine_features(key, part):
    return banded_field(jax.random.fold_in(key, 11), IMAGES, C4, H4, COLS).astype(jnp.bfloat16)


def draw_coarse_level(key, part):
    return banded_field(jax.random.fold_in(key, 12), IMAGES, D, H4 // 2, COLS // 2).astype(jnp.bfloat16)


def draw_queries(key, part):
    key_base = jax.random.fold_in(jax.random.fold_in(key, 13), 0)
    values = 0.25 * jax.random.truncated_normal(key_base, -4.0, 4.0, (QUERIES, D), jnp.float32)
    return values.astype(jnp.bfloat16)


def levels(own_key, extent, shards, smallest, high):
    factor_of = 1.0
    for axis_at, parts in shards:
        heights = jax.random.uniform(jax.random.fold_in(jax.random.fold_in(own_key, 6), axis_at), (parts,), jnp.float32, smallest / len(shards), high / len(shards))
        factor_of = factor_of * jnp.repeat(jnp.exp(heights), extent[axis_at] // parts).reshape((-1,) + (1,) * (len(extent) - 1 - axis_at))
    return factor_of


def bell_draw(stream_key, shape, spread, most, pieces=(), kind=jnp.bfloat16):
    values = jax.random.normal(stream_key, shape, jnp.float32) * spread
    if len(pieces) > 0:
        values = levels(stream_key, shape, pieces, -0.22, 0.18) * values
    return jnp.clip(values, min=-most, max=most).astype(kind)


def setup_inputs(seed: int = 0) -> dict:
    key_of = jax.random.split(jax.random.key(seed), 12)
    return {
        "fine_features": draw_fine_features(jax.random.fold_in(key_of[11], 71), 0),
        "coarse_level": draw_coarse_level(jax.random.fold_in(key_of[11], 71), 0),
        "lat_weight": bell_draw(key_of[2], (D, C4), C4 ** -0.5, 0.4375, ((0, 2),)),
        "lat_gain": jnp.clip(1.0 + 0.18 * jax.random.normal(key_of[3], (D,), jnp.float32), 0.099609375, 1.8984375).astype(jnp.bfloat16),
        "lat_shift": bell_draw(key_of[4], (D,), 0.5, 3.0, ((0, 2),)),
        "out_weight": bell_draw(key_of[5], (3, 3, D, D), (9 * D) ** -0.5, 0.125, ((2, 2),)),
        "out_gain": jnp.clip(1.0 + 0.18 * jax.random.normal(key_of[6], (D,), jnp.float32), 0.099609375, 1.8984375).astype(jnp.bfloat16),
        "out_shift": bell_draw(key_of[7], (D,), 0.5, 3.0, ((0, 2),)),
        "mask_weight": bell_draw(key_of[8], (D, D), D ** -0.5, 0.375, ((0, 2),)),
        "mask_bias": bell_draw(key_of[9], (D,), 0.3, 1.796875, ((0, 2),)),
        "queries": draw_queries(jax.random.fold_in(key_of[11], 71), 0),
    }


epsilon = 1e-05

def interp(padded, axis):
    length = padded.shape[axis] - 2
    before = lax.slice_in_dim(padded, 0, length, axis=axis)
    middle = lax.slice_in_dim(padded, 1, length + 1, axis=axis)
    after = lax.slice_in_dim(padded, 2, length + 2, axis=axis)
    even_part = 0.25 * before + 0.75 * middle
    odd_part = 0.75 * middle + 0.25 * after
    paired = jnp.stack([even_part, odd_part], axis + 1)
    new_shape = list(middle.shape)
    new_shape[axis] = 2 * length
    return paired.reshape(new_shape)

def group_norm(values, gain, shift, group_size):
    channels, height, width = values.shape
    blocks = values.reshape(channels // group_size, group_size * height * width)
    mean_value = lax.optimization_barrier(jnp.mean(blocks, axis=1, keepdims=True))
    deviation = blocks - mean_value
    variance = lax.optimization_barrier(jnp.mean(deviation * deviation, axis=1, keepdims=True))
    scaled = ((blocks - mean_value) * lax.rsqrt(variance + epsilon)).reshape(channels, height, width)
    return scaled * gain.astype(jnp.float32)[:, None, None] + shift.astype(jnp.float32)[:, None, None]

def reference(fine_features, coarse_level, lat_weight, lat_gain, lat_shift, out_weight, out_gain, out_shift, mask_weight, mask_bias, queries):
    group_size = D // GROUPS

    def one_image(pair):
        fine_image, coarse_image = pair
        lateral = jnp.dot(lat_weight, fine_image.reshape(C4, H4 * COLS), preferred_element_type=jnp.float32).reshape(D, H4, COLS)
        lat_normed = group_norm(lateral, lat_gain, lat_shift, group_size)
        extended = jnp.pad(coarse_image.astype(jnp.float32), ((0, 0), (1, 1), (1, 1)), mode='edge')
        upsampled = interp(interp(extended, 1), 2)
        joined = (lat_normed + upsampled).astype(jnp.bfloat16)
        padded = jnp.pad(joined, ((0, 0), (1, 1), (1, 1)))
        conv_out = jnp.zeros((D, H4 * COLS), jnp.float32)
        for row_tap in range(3):
            for col_tap in range(3):
                window = padded[:, row_tap:row_tap + H4, col_tap:col_tap + COLS].reshape(D, H4 * COLS)
                conv_out = conv_out + jnp.dot(out_weight[row_tap, col_tap], window, preferred_element_type=jnp.float32)
        conv_out = conv_out.reshape(D, H4, COLS)
        activated = jnp.maximum(group_norm(conv_out, out_gain, out_shift, group_size), 0.0).astype(jnp.bfloat16)
        features = jnp.dot(mask_weight, activated.reshape(D, H4 * COLS), preferred_element_type=jnp.float32)
        features = (features + mask_bias.astype(jnp.float32)[:, None]).astype(jnp.bfloat16)
        logits = jnp.dot(queries, features, preferred_element_type=jnp.float32)
        peak = lax.optimization_barrier(jnp.max(logits, axis=0, keepdims=True))
        shifted = logits - peak
        result = shifted - jnp.log(lax.optimization_barrier(jnp.sum(jnp.exp(shifted), axis=0, keepdims=True)))
        return result.reshape(QUERIES, H4, COLS)
    return lax.map(one_image, (fine_features, coarse_level))
```

```python
import functools

import jax
import jax.numpy as jnp
from jax import lax
from jax.experimental import pallas as pl
from jax.experimental.pallas import tpu as pltpu
from jax.sharding import PartitionSpec as P

D = 256
GROUPS = 32
EPS = 1e-05
MESH = pl.DeviceIdType.MESH
F32 = jnp.float32
BF16 = jnp.bfloat16


def wait_on(ref, sem):
    pltpu.make_async_copy(ref, ref, sem).wait()


def kernel(
    bands, chans, pixel_count,
    fine, coarse, early, late, queries,
    out,
    feats, level, ebuf, lbuf, lat, cols_up, stacked, conv, rows_out, stat1, stat2,
    f_send, f_recv, fh_send, fh_recv, c_send, c_recv, ch_send, ch_recv,
    w_send, w_recv, s_send, s_recv, o_sem,
):
    images, band_rows, in_ch, width = fine.shape
    rows = band_rows // chans
    c_rows = coarse.shape[1] // chans
    c_ch = coarse.shape[2]
    share = early.shape[0]
    gsize = D // GROUPS
    total = bands * chans
    b = lax.axis_index("band")
    c = lax.axis_index("chan")
    me = b * chans + c
    sends = []

    def send(src, dst, ssem, rsem, tb, tc, maybe_self):
        def remote():
            return pltpu.make_async_remote_copy(
                src_ref=src, dst_ref=dst, send_sem=ssem, recv_sem=rsem,
                device_id=(tb, tc), device_id_type=MESH,
            )

        if not maybe_self:
            remote().start()
            sends.append((remote, None))
            return
        is_self = jnp.logical_and(tb == b, tc == c)

        @pl.when(is_self)
        def _():
            pltpu.make_async_copy(src, dst, rsem).start()

        @pl.when(jnp.logical_not(is_self))
        def _():
            remote().start()

        sends.append((remote, is_self))

    def block(index, size):
        return pl.ds(pl.multiple_of(index * size, size), size)

    def gather(src, dst, ssem, rsem):
        pltpu.make_async_copy(src, dst.at[block(c, share)], rsem.at[0]).start()
        for s in range(1, chans):
            t = lax.rem(c + s, chans)
            send(src, dst.at[block(c, share)], ssem.at[s], rsem.at[s], b, t, False)

    def main_rows(src, dst, n, size, ch, ssem, rsem):
        for s in range(chans):
            t = lax.rem(c + s, chans)
            piece = src.at[n, pl.ds(t * size, size)]
            place = dst.at[n, pl.ds(1, size), block(c, ch)]
            if s == 0:
                pltpu.make_async_copy(piece, place, rsem.at[n, 0]).start()
            else:
                send(piece, place, ssem.at[n, s], rsem.at[n, s], b, t, False)

    def halo_rows(src, dst, n, size, ch, ssem, rsem):
        for s in range(chans):
            t = lax.rem(c + s, chans)
            k = (s + 1) % chans
            to = lax.rem(b * chans + t + 1, total)
            send(
                src.at[n, (t + 1) * size - 1], dst.at[n, 0, block(c, ch)],
                ssem.at[n, 0, s], rsem.at[n, 0, k], to // chans, lax.rem(to, chans), k == 0,
            )
            k = (s - 1) % chans
            to = lax.rem(b * chans + t - 1 + total, total)
            send(
                src.at[n, t * size], dst.at[n, size + 1, block(c, ch)],
                ssem.at[n, 1, s], rsem.at[n, 1, k], to // chans, lax.rem(to, chans), k == 0,
            )

    def wait_main(dst, n, size, ch, rsem):
        for s in range(chans):
            wait_on(dst.at[n, pl.ds(1, size), pl.ds(0, ch)], rsem.at[n, s])

    def wait_halo(dst, n, size, ch, rsem):
        for side in range(2):
            for s in range(chans):
                wait_on(dst.at[n, side * (size + 1), pl.ds(0, ch)], rsem.at[n, side, s])

    gather(early, ebuf, w_send.at[0], w_recv.at[0])
    for n in range(images):
        main_rows(fine, feats, n, rows, in_ch, f_send, f_recv)
    for n in range(images):
        halo_rows(fine, feats, n, rows, in_ch, fh_send, fh_recv)
        main_rows(coarse, level, n, c_rows, c_ch, c_send, c_recv)
        halo_rows(coarse, level, n, c_rows, c_ch, ch_send, ch_recv)
        if n == 0:
            gather(late, lbuf, w_send.at[1], w_recv.at[1])

    local_count = float(gsize * rows * width)
    lane = lax.broadcasted_iota(jnp.int32, (GROUPS, 128), 1)
    sub = lax.broadcasted_iota(jnp.int32, (GROUPS, 128), 0)
    eye = lane == sub
    tile_row = lax.broadcasted_iota(jnp.int32, (8, 128), 0)

    def group_sum(x):
        x = jnp.sum(x.reshape(GROUPS, gsize, x.shape[1]), axis=1)
        return jnp.sum(x, axis=1, keepdims=True)

    def to_channels(col):
        return jnp.broadcast_to(col[:, None, :], (GROUPS, gsize, 1)).reshape(D, 1)

    def to_row(col):
        return jnp.sum(jnp.where(eye, jnp.broadcast_to(col, (GROUPS, 128)), 0.0), axis=0, keepdims=True)

    def to_col(row):
        return jnp.sum(jnp.where(eye, jnp.broadcast_to(row, (GROUPS, 128)), 0.0), axis=1, keepdims=True)

    def local_stats(ref, n, first):
        s = group_sum(lax.fori_loop(
            0, rows, lambda r, acc: acc + ref[n, r + first], jnp.zeros((D, width), F32)))
        mean = to_channels(s / local_count)

        def step(r, acc):
            d = ref[n, r + first] - mean
            return acc + d * d

        m2 = group_sum(lax.fori_loop(0, rows, step, jnp.zeros((D, width), F32)))
        return to_row(s), to_row(m2)

    def exchange(stats, buf, which):
        tile = jnp.zeros((8, 128), F32)
        for n in range(images):
            for kind in range(2):
                tile = jnp.where(tile_row == kind * images + n, stats[n][kind], tile)
        buf[0] = tile

        def one(k, carry):
            to = lax.rem(me + k, total)
            pltpu.make_async_remote_copy(
                src_ref=buf.at[0], dst_ref=buf.at[k],
                send_sem=s_send.at[which], recv_sem=s_recv.at[which],
                device_id=(to // chans, lax.rem(to, chans)), device_id_type=MESH,
            ).start()
            return carry

        lax.fori_loop(1, total, one, 0)

    def combined(buf, which):
        wait_on(buf.at[pl.ds(1, total - 1)], s_recv.at[which])
        sums = buf[:, 0:images, :]
        m2s = buf[:, images:2 * images, :]
        mean = jnp.sum(sums, axis=0) / pixel_count
        off = sums / local_count - mean[None]
        var = (jnp.sum(m2s, axis=0) + local_count * jnp.sum(off * off, axis=0)) / pixel_count
        inv = lax.rsqrt(var + EPS)
        return [
            (to_channels(to_col(mean[n:n + 1])), to_channels(to_col(inv[n:n + 1])))
            for n in range(images)
        ]

    for s in range(chans):
        wait_on(ebuf.at[pl.ds(0, share)], w_recv.at[0, s])
    lat_w = ebuf[:, 0:in_ch * chans]
    params = ebuf[:, D:D + 128].astype(F32)
    lat_gain, lat_shift, out_gain, out_shift, bias = (params[:, k:k + 1] for k in range(5))

    stats = []
    for n in range(images):
        wait_main(feats, n, rows, in_ch, f_recv)

        def lateral(r, carry):
            lat[n, r + 1] = jnp.dot(lat_w, feats[n, r + 1], preferred_element_type=F32)
            return carry

        lax.fori_loop(0, rows, lateral, 0)
        stats.append(local_stats(lat, n, 1))
    exchange(stats, stat1, 0)

    src_col = lax.broadcasted_iota(jnp.int32, (width // 2, width), 0)
    dst_col = lax.broadcasted_iota(jnp.int32, (width // 2, width), 1)
    half = dst_col // 2
    near = jnp.where(src_col == half, 0.75, 0.0)
    other = jnp.clip(jnp.where(dst_col - 2 * half == 0, half - 1, half + 1), 0, width // 2 - 1)
    up = (near + jnp.where(src_col == other, 0.25, 0.0)).astype(BF16)
    lane_w = lax.broadcasted_iota(jnp.int32, (D, width), 1)

    norms = None
    for n in range(images):
        wait_halo(feats, n, rows, in_ch, fh_recv)
        for j in (0, rows + 1):
            lat[n, j] = jnp.dot(lat_w, feats[n, j], preferred_element_type=F32)
        wait_main(level, n, c_rows, c_ch, c_recv)
        wait_halo(level, n, c_rows, c_ch, ch_recv)

        def widen(k, carry):
            cols_up[k] = jnp.dot(level[n, k], up, preferred_element_type=F32)
            return carry

        lax.fori_loop(0, c_rows + 2, widen, 0)

        @pl.when(me == 0)
        def _():
            cols_up[0] = cols_up[1]

        @pl.when(me == total - 1)
        def _():
            cols_up[c_rows + 1] = cols_up[c_rows]

        if norms is None:
            norms = combined(stat1, 0)
        mean, inv = norms[n]
        scale = inv * lat_gain

        def join(j, carry):
            k = j // 2
            even = j - 2 * k == 0
            w0 = jnp.where(even, 0.75, 0.25)
            w1 = jnp.where(even, 0.25, 0.75)
            upsampled = w0 * cols_up[k] + w1 * cols_up[k + 1]
            joined = (lat[n, j] - mean) * scale + lat_shift + upsampled
            inside = jnp.logical_and(me * rows + j >= 1, me * rows + j <= total * rows)
            joined = jnp.where(inside, joined, 0.0)
            left = jnp.where(lane_w == 0, 0.0, pltpu.roll(joined, 1, 1))
            right = jnp.where(lane_w == width - 1, 0.0, pltpu.roll(joined, width - 1, 1))
            base = pl.multiple_of(j * 3 * D, D)
            stacked[pl.ds(base, D)] = left.astype(BF16)
            stacked[pl.ds(base + D, D)] = joined.astype(BF16)
            stacked[pl.ds(base + 2 * D, D)] = right.astype(BF16)
            return carry

        lax.fori_loop(0, rows + 2, join, 0)
        if n == 0:
            for s in range(chans):
                wait_on(lbuf.at[pl.ds(0, share)], w_recv.at[1, s])

        def convolve(r, carry):
            base = pl.multiple_of(r * 3 * D, D)
            conv[n, r] = jnp.dot(
                lbuf[:, 0:9 * D], stacked[pl.ds(base, 9 * D)], preferred_element_type=F32)
            return carry

        lax.fori_loop(0, rows, convolve, 0)

    exchange([local_stats(conv, n, 0) for n in range(images)], stat2, 1)
    norms = combined(stat2, 1)
    for n in range(images):
        mean, inv = norms[n]
        scale = inv * out_gain

        def finish(r, carry):
            act = jnp.maximum((conv[n, r] - mean) * scale + out_shift, 0.0).astype(BF16)
            mixed = jnp.dot(lbuf[:, 9 * D:10 * D], act, preferred_element_type=F32)
            features = (mixed + bias).astype(BF16)
            logits = jnp.dot(queries[...], features, preferred_element_type=F32)
            shifted = logits - jnp.max(logits, axis=0, keepdims=True)
            norm = jnp.log(jnp.sum(jnp.exp(shifted), axis=0, keepdims=True))
            rows_out[n, r] = shifted - norm
            pltpu.make_async_copy(rows_out.at[n, r], out.at[n, r], o_sem.at[n, r]).start()
            return carry

        lax.fori_loop(0, rows, finish, 0)

    for n in range(images):
        for r in range(rows):
            pltpu.make_async_copy(rows_out.at[n, r], out.at[n, r], o_sem.at[n, r]).wait()
    for which, buf in ((0, stat1), (1, stat2)):
        wait_on(buf.at[pl.ds(1, total - 1)], s_send.at[which])
    for remote, is_self in sends:
        if is_self is None:
            remote().wait_send()
        else:
            @pl.when(jnp.logical_not(is_self))
            def _():
                remote().wait_send()


def per_device(
    bands, chans,
    fine_features, coarse_level, lat_weight, lat_gain, lat_shift, out_weight, out_gain, out_shift,
    mask_weight, mask_bias, queries,
):
    images, in_ch, band_rows, width = fine_features.shape
    share = lat_weight.shape[0]
    c_ch, c_band = coarse_level.shape[1], coarse_level.shape[2]
    rows, c_rows = band_rows // chans, c_band // chans
    query_count = queries.shape[0]
    pixel_count = float(D // GROUPS * band_rows * bands * width)
    fine = jnp.transpose(fine_features, (0, 2, 1, 3))
    coarse = jnp.transpose(coarse_level, (0, 2, 1, 3))
    params = jnp.stack([lat_gain, lat_shift, out_gain, out_shift, mask_bias], axis=1)
    early = jnp.concatenate([
        jnp.pad(lat_weight, ((0, 0), (0, D - lat_weight.shape[1]))),
        jnp.pad(params, ((0, 0), (0, 128 - params.shape[1]))),
    ], axis=1)
    late = jnp.concatenate([
        jnp.transpose(out_weight, (2, 0, 1, 3)).reshape(share, 9 * D), mask_weight,
    ], axis=1)
    anywhere = pl.BlockSpec(memory_space=pl.ANY)
    vmem = pl.BlockSpec(memory_space=pltpu.VMEM)
    dma = pltpu.SemaphoreType.DMA
    result = pl.pallas_call(
        functools.partial(kernel, bands, chans, pixel_count),
        out_shape=jax.ShapeDtypeStruct((images, rows, query_count, width), F32),
        in_specs=[anywhere, anywhere, anywhere, anywhere, vmem],
        out_specs=anywhere,
        scratch_shapes=[
            pltpu.VMEM((images, rows + 2, chans * in_ch, width), BF16),
            pltpu.VMEM((images, c_rows + 2, chans * c_ch, width // 2), BF16),
            pltpu.VMEM((chans * share, early.shape[1]), BF16),
            pltpu.VMEM((chans * share, late.shape[1]), BF16),
            pltpu.VMEM((images, rows + 2, D, width), F32),
            pltpu.VMEM((c_rows + 2, D, width), F32),
            pltpu.VMEM(((rows + 2) * 3 * D, width), BF16),
            pltpu.VMEM((images, rows, D, width), F32),
            pltpu.VMEM((images, rows, query_count, width), F32),
            pltpu.VMEM((bands * chans, 8, 128), F32),
            pltpu.VMEM((bands * chans, 8, 128), F32),
            dma((images, chans)), dma((images, chans)),
            dma((images, 2, chans)), dma((images, 2, chans)),
            dma((images, chans)), dma((images, chans)),
            dma((images, 2, chans)), dma((images, 2, chans)),
            dma((2, chans)), dma((2, chans)),
            dma((2,)), dma((2,)),
            dma((images, rows)),
        ],
        compiler_params=pltpu.CompilerParams(
            has_side_effects=True, vmem_limit_bytes=60 * 1024 * 1024),
    )(fine, coarse, early, late, queries)
    return jnp.transpose(result, (0, 2, 1, 3))


def solution(mesh):
    return jax.shard_map(
        functools.partial(per_device, mesh.shape["band"], mesh.shape["chan"]),
        mesh=mesh,
        in_specs=(
            P(None, "chan", "band", None),
            P(None, "chan", "band", None),
            P("chan", None),
            P("chan"),
            P("chan"),
            P(None, None, "chan", None),
            P("chan"),
            P("chan"),
            P("chan", None),
            P("chan"),
            P(),
        ),
        out_specs=P(None, None, ("band", "chan"), None),
        check_vma=False,
    )
```

```python
import functools
import math

import jax
import jax.numpy as jnp
from jax import lax
from jax.experimental import pallas as pl
from jax.experimental.pallas import tpu as pltpu
from jax.sharding import PartitionSpec as P

D = 256
GROUPS = 32
EPS = 1e-05
MESH = pl.DeviceIdType.MESH
F32 = jnp.float32
BF16 = jnp.bfloat16


def wait_on(ref, sem):
    pltpu.make_async_copy(ref, ref, sem).wait()


def kernel(
    bands, chans, pixel_count,
    fine, coarse, lat_in, par_in, conv_in, mask_in, queries,
    out,
    feats, level, ebuf, pbuf, wbuf, mbuf, wide, lat, cols_up, stacked, conv, rows_out, stat1, stat2,
    f_send, f_recv, fh_send, fh_recv, c_send, c_recv, ch_send, ch_recv,
    e_send, e_recv, w_send, w_recv, q_send, q_recv, s_send, s_recv, o_sem,
):
    images, band_rows, in_ch, width = fine.shape
    rows = band_rows // chans
    c_rows = coarse.shape[1] // chans
    c_ch = coarse.shape[2]
    share = lat_in.shape[1]
    quad = math.gcd(bands, 4)
    quarter = share // quad
    gsize = D // GROUPS
    total = bands * chans
    b = lax.axis_index("band")
    c = lax.axis_index("chan")
    me = b * chans + c
    sends = []

    def send(src, dst, ssem, rsem, tb, tc, maybe_self):
        def remote():
            return pltpu.make_async_remote_copy(
                src_ref=src, dst_ref=dst, send_sem=ssem, recv_sem=rsem,
                device_id=(tb, tc), device_id_type=MESH,
            )

        if not maybe_self:
            remote().start()
            sends.append((remote, None))
            return
        is_self = jnp.logical_and(tb == b, tc == c)

        @pl.when(is_self)
        def _():
            pltpu.make_async_copy(src, dst, rsem).start()

        @pl.when(jnp.logical_not(is_self))
        def _():
            remote().start()

        sends.append((remote, is_self))

    def block(index, size):
        return pl.ds(pl.multiple_of(index * size, size), size)

    def gather(src, dst, ssem, rsem):
        pltpu.make_async_copy(src, dst.at[c], rsem.at[0]).start()
        for s in range(1, chans):
            t = lax.rem(c + s, chans)
            send(src, dst.at[c], ssem.at[s], rsem.at[s], b, t, False)

    spot = lax.rem(b, quad)

    def quarter_of(owner, part):
        return pl.ds(pl.multiple_of(owner * share + part * quarter, quarter), quarter)

    def weights_across(src, dst, ssem, rsem):
        pltpu.make_async_copy(src, dst.at[:, block(c, share)], rsem.at[0]).start()
        for s in range(1, chans):
            t = lax.rem(c + s, chans)
            send(
                src.at[:, pl.ds(pl.multiple_of(spot * quarter, quarter), quarter)],
                dst.at[:, quarter_of(c, spot)], ssem.at[s], rsem.at[s], b, t, False,
            )

    def weights_around(dst, rsem, ssem2, rsem2):
        for s in range(1, chans):
            wait_on(dst.at[:, pl.ds(0, quarter)], rsem.at[s])
            owner = lax.rem(c - s + chans, chans)
            piece = dst.at[:, quarter_of(owner, spot)]
            for m in range(1, quad):
                mate = b - spot + lax.rem(spot + m, quad)
                send(piece, piece, ssem2.at[s, m], rsem2.at[s, m], mate, c, False)

    def wait_weights(dst, rsem, rsem2):
        wait_on(dst.at[:, pl.ds(0, share)], rsem.at[0])
        for s in range(1, chans):
            for m in range(1, quad):
                wait_on(dst.at[:, pl.ds(0, quarter)], rsem2.at[s, m])

    def main_rows(src, dst, n, size, ch, ssem, rsem):
        for s in range(chans):
            t = lax.rem(c + s, chans)
            piece = src.at[n, pl.ds(t * size, size)]
            place = dst.at[n, pl.ds(1, size), block(c, ch)]
            if s == 0:
                pltpu.make_async_copy(piece, place, rsem.at[n, 0]).start()
            else:
                send(piece, place, ssem.at[n, s], rsem.at[n, s], b, t, False)

    def halo_rows(src, dst, n, size, ch, ssem, rsem):
        for s in range(chans):
            t = lax.rem(c + s, chans)
            k = (s + 1) % chans
            to = lax.rem(b * chans + t + 1, total)
            send(
                src.at[n, (t + 1) * size - 1], dst.at[n, 0, block(c, ch)],
                ssem.at[n, 0, s], rsem.at[n, 0, k], to // chans, lax.rem(to, chans), k == 0,
            )
            k = (s - 1) % chans
            to = lax.rem(b * chans + t - 1 + total, total)
            send(
                src.at[n, t * size], dst.at[n, size + 1, block(c, ch)],
                ssem.at[n, 1, s], rsem.at[n, 1, k], to // chans, lax.rem(to, chans), k == 0,
            )

    def wait_main(dst, n, size, ch, rsem):
        for s in range(chans):
            wait_on(dst.at[n, pl.ds(1, size), pl.ds(0, ch)], rsem.at[n, s])

    def wait_halo(dst, n, size, ch, rsem):
        for side in range(2):
            for s in range(chans):
                wait_on(dst.at[n, side * (size + 1), pl.ds(0, ch)], rsem.at[n, side, s])

    gather(lat_in, ebuf, e_send.at[0], e_recv.at[0])
    gather(par_in, pbuf, e_send.at[1], e_recv.at[1])
    for n in range(images):
        main_rows(fine, feats, n, rows, in_ch, f_send, f_recv)
    weights_across(conv_in, wbuf, w_send.at[0], w_recv.at[0])
    weights_across(mask_in, mbuf, w_send.at[1], w_recv.at[1])
    halo_rows(fine, feats, 0, rows, in_ch, fh_send, fh_recv)

    local_count = float(gsize * rows * width)
    lane = lax.broadcasted_iota(jnp.int32, (GROUPS, 128), 1)
    sub = lax.broadcasted_iota(jnp.int32, (GROUPS, 128), 0)

    def fold(x):
        acc = x[:, 0:128]
        for k in range(1, width // 128):
            acc = acc + x[:, k * 128:(k + 1) * 128]
        return acc

    def group_sum(x):
        x = jnp.sum(x.reshape(GROUPS, gsize, x.shape[1]), axis=1)
        return jnp.sum(x, axis=1, keepdims=True)

    def to_channels(col):
        return jnp.broadcast_to(col[:, None, :], (GROUPS, gsize, 1)).reshape(D, 1)

    def at_lanes(col, slot):
        return jnp.where(lane == sub + slot * GROUPS, jnp.broadcast_to(col, (GROUPS, 128)), 0.0)

    def from_lanes(row, slot):
        spread = jnp.where(lane == sub + slot * GROUPS, jnp.broadcast_to(row, (GROUPS, 128)), 0.0)
        return jnp.sum(spread, axis=1, keepdims=True)

    def produce(ref, n, first, compute):
        def step(r, acc):
            y = compute(r)
            ref[n, r + first] = y
            return acc + fold(y)

        s = group_sum(lax.fori_loop(0, rows, step, jnp.zeros((D, 128), F32)))
        mean = to_channels(s / local_count)

        def spread(r, acc):
            d = ref[n, r + first] - mean
            return acc + fold(d * d)

        m2 = group_sum(lax.fori_loop(0, rows, spread, jnp.zeros((D, 128), F32)))
        return at_lanes(s, n) + at_lanes(m2, images + n)

    def exchange(stats, buf, which):
        buf[0] = jnp.sum(stats, axis=0, keepdims=True)

        def one(k, carry):
            to = lax.rem(me + k, total)
            pltpu.make_async_remote_copy(
                src_ref=buf.at[0], dst_ref=buf.at[k],
                send_sem=s_send.at[which], recv_sem=s_recv.at[which],
                device_id=(to // chans, lax.rem(to, chans)), device_id_type=MESH,
            ).start()
            return carry

        lax.fori_loop(1, total, one, 0)

    def combined(buf, which):
        wait_on(buf.at[pl.ds(1, total - 1)], s_recv.at[which])
        parts = buf[...]
        sums = jnp.sum(parts, axis=0)
        mean = sums / pixel_count
        off = parts / local_count - mean[None]
        m2 = pltpu.roll(sums, 128 - images * GROUPS, 1)
        var = (m2 + local_count * jnp.sum(off * off, axis=0)) / pixel_count
        inv = lax.rsqrt(var + EPS)
        return [
            (to_channels(from_lanes(mean, n)), to_channels(from_lanes(inv, n)))
            for n in range(images)
        ]

    for k in range(2):
        for s in range(chans):
            wait_on((ebuf, pbuf)[k].at[0], e_recv.at[k, s])
    square = (
        lax.broadcasted_iota(jnp.int32, (share, share), 0)
        == lax.broadcasted_iota(jnp.int32, (share, share), 1)
    )

    def column(k):
        return jnp.concatenate([
            jnp.sum(jnp.where(
                square, jnp.broadcast_to(pbuf[s].astype(F32)[k:k + 1], (share, share)), 0.0,
            ), axis=1, keepdims=True)
            for s in range(chans)
        ], axis=0)

    lat_gain, lat_shift, out_gain, out_shift, bias = (column(k) for k in range(5))

    def lateral(features):
        return jnp.concatenate([
            lax.dot_general(
                ebuf[s], features, (((0,), (0,)), ((), ())), preferred_element_type=F32)
            for s in range(chans)
        ], axis=0)

    stats = jnp.zeros((GROUPS, 128), F32)
    for n in range(images):
        wait_main(feats, n, rows, in_ch, f_recv)
        stats = stats + produce(lat, n, 1, lambda r, n=n: lateral(feats[n, r + 1]))
    exchange(stats, stat1, 0)
    for n in range(images):
        if n > 0:
            halo_rows(fine, feats, n, rows, in_ch, fh_send, fh_recv)
        main_rows(coarse, level, n, c_rows, c_ch, c_send, c_recv)
        halo_rows(coarse, level, n, c_rows, c_ch, ch_send, ch_recv)
    weights_around(wbuf, w_recv.at[0], q_send.at[0], q_recv.at[0])
    weights_around(mbuf, w_recv.at[1], q_send.at[1], q_recv.at[1])

    src_col = lax.broadcasted_iota(jnp.int32, (width // 2, width), 0)
    dst_col = lax.broadcasted_iota(jnp.int32, (width // 2, width), 1)
    half = dst_col // 2
    near = jnp.where(src_col == half, 0.75, 0.0)
    other = jnp.clip(jnp.where(dst_col - 2 * half == 0, half - 1, half + 1), 0, width // 2 - 1)
    up = (near + jnp.where(src_col == other, 0.25, 0.0)).astype(BF16)
    lane_w = lax.broadcasted_iota(jnp.int32, (D, width), 1)

    stats = jnp.zeros((GROUPS, 128), F32)
    norms = None
    for n in range(images):
        wait_halo(feats, n, rows, in_ch, fh_recv)
        for j in (0, rows + 1):
            lat[n, j] = lateral(feats[n, j])
        wait_main(level, n, c_rows, c_ch, c_recv)
        wait_halo(level, n, c_rows, c_ch, ch_recv)

        def widen(k, carry):
            cols_up[k] = jnp.dot(level[n, k], up, preferred_element_type=F32)
            return carry

        lax.fori_loop(0, c_rows + 2, widen, 0)

        @pl.when(me == 0)
        def _():
            cols_up[0] = cols_up[1]

        @pl.when(me == total - 1)
        def _():
            cols_up[c_rows + 1] = cols_up[c_rows]

        if norms is None:
            norms = combined(stat1, 0)
        mean, inv = norms[n]
        scale = inv * lat_gain

        def join(j, carry):
            k = j // 2
            even = j - 2 * k == 0
            w0 = jnp.where(even, 0.75, 0.25)
            w1 = jnp.where(even, 0.25, 0.75)
            upsampled = w0 * cols_up[k] + w1 * cols_up[k + 1]
            joined = (lat[n, j] - mean) * scale + lat_shift + upsampled
            inside = jnp.logical_and(me * rows + j >= 1, me * rows + j <= total * rows)
            joined = jnp.where(inside, joined, 0.0)
            left = jnp.where(lane_w == 0, 0.0, pltpu.roll(joined, 1, 1))
            right = jnp.where(lane_w == width - 1, 0.0, pltpu.roll(joined, width - 1, 1))
            base = pl.multiple_of(j * 3 * D, D)
            stacked[pl.ds(base, D)] = left.astype(BF16)
            stacked[pl.ds(base + D, D)] = joined.astype(BF16)
            stacked[pl.ds(base + 2 * D, D)] = right.astype(BF16)
            return carry

        lax.fori_loop(0, rows + 2, join, 0)
        if n == 0:
            wait_weights(wbuf, w_recv.at[0], q_recv.at[0])
            for k in range(9):
                wide[:, k * D:(k + 1) * D] = wbuf[k]

        def convolve(r):
            base = pl.multiple_of(r * 3 * D, D)
            return jnp.dot(wide[...], stacked[pl.ds(base, 9 * D)], preferred_element_type=F32)

        stats = stats + produce(conv, n, 0, convolve)

    exchange(stats, stat2, 1)
    wait_weights(mbuf, w_recv.at[1], q_recv.at[1])
    norms = combined(stat2, 1)
    for n in range(images):
        mean, inv = norms[n]
        scale = inv * out_gain

        def finish(r, carry):
            act = jnp.maximum((conv[n, r] - mean) * scale + out_shift, 0.0).astype(BF16)
            mixed = jnp.dot(mbuf[0], act, preferred_element_type=F32)
            features = (mixed + bias).astype(BF16)
            logits = jnp.dot(queries[...], features, preferred_element_type=F32)
            shifted = logits - jnp.max(logits, axis=0, keepdims=True)
            norm = jnp.log(jnp.sum(jnp.exp(shifted), axis=0, keepdims=True))
            rows_out[n, r] = shifted - norm
            pltpu.make_async_copy(rows_out.at[n, r], out.at[n, r], o_sem.at[n, r]).start()
            return carry

        lax.fori_loop(0, rows, finish, 0)

    for n in range(images):
        for r in range(rows):
            pltpu.make_async_copy(rows_out.at[n, r], out.at[n, r], o_sem.at[n, r]).wait()
    for which, buf in ((0, stat1), (1, stat2)):
        wait_on(buf.at[pl.ds(1, total - 1)], s_send.at[which])
    for remote, is_self in sends:
        if is_self is None:
            remote().wait_send()
        else:
            @pl.when(jnp.logical_not(is_self))
            def _():
                remote().wait_send()


def per_device(
    bands, chans,
    fine_features, coarse_level, lat_weight, lat_gain, lat_shift, out_weight, out_gain, out_shift,
    mask_weight, mask_bias, queries,
):
    images, in_ch, band_rows, width = fine_features.shape
    share = lat_weight.shape[0]
    c_ch, c_band = coarse_level.shape[1], coarse_level.shape[2]
    rows, c_rows = band_rows // chans, c_band // chans
    query_count = queries.shape[0]
    pixel_count = float(D // GROUPS * band_rows * bands * width)
    fine = jnp.transpose(fine_features, (0, 2, 1, 3))
    coarse = jnp.transpose(coarse_level, (0, 2, 1, 3))
    params = jnp.stack([lat_gain, lat_shift, out_gain, out_shift, mask_bias], axis=0)
    params = jnp.pad(params, ((0, 16 - params.shape[0]), (0, 0)))
    anywhere = pl.BlockSpec(memory_space=pl.ANY)
    vmem = pl.BlockSpec(memory_space=pltpu.VMEM)
    dma = pltpu.SemaphoreType.DMA
    result = pl.pallas_call(
        functools.partial(kernel, bands, chans, pixel_count),
        out_shape=jax.ShapeDtypeStruct((images, rows, query_count, width), F32),
        in_specs=[anywhere] * 6 + [vmem],
        out_specs=anywhere,
        scratch_shapes=[
            pltpu.VMEM((images, rows + 2, chans * in_ch, width), BF16),
            pltpu.VMEM((images, c_rows + 2, chans * c_ch, width // 2), BF16),
            pltpu.VMEM((chans, chans * in_ch, share), BF16),
            pltpu.VMEM((chans, 16, share), BF16),
            pltpu.VMEM((9, D, D), BF16),
            pltpu.VMEM((1, D, D), BF16),
            pltpu.VMEM((D, 9 * D), BF16),
            pltpu.VMEM((images, rows + 2, D, width), F32),
            pltpu.VMEM((c_rows + 2, D, width), F32),
            pltpu.VMEM(((rows + 2) * 3 * D, width), BF16),
            pltpu.VMEM((images, rows, D, width), F32),
            pltpu.VMEM((images, rows, query_count, width), F32),
            pltpu.VMEM((bands * chans, 1, 128), F32),
            pltpu.VMEM((bands * chans, 1, 128), F32),
            dma((images, chans)), dma((images, chans)),
            dma((images, 2, chans)), dma((images, 2, chans)),
            dma((images, chans)), dma((images, chans)),
            dma((images, 2, chans)), dma((images, 2, chans)),
            dma((2, chans)), dma((2, chans)), dma((2, chans)), dma((2, chans)),
            dma((2, chans, 4)), dma((2, chans, 4)),
            dma((2,)), dma((2,)),
            dma((images, rows)),
        ],
        compiler_params=pltpu.CompilerParams(
            has_side_effects=True, vmem_limit_bytes=60 * 1024 * 1024),
    )(
        fine, coarse, lat_weight.T, params, out_weight.reshape(9, share, D), mask_weight[None],
        queries,
    )
    return jnp.transpose(result, (0, 2, 1, 3))


def solution(mesh):
    return jax.shard_map(
        functools.partial(per_device, mesh.shape["band"], mesh.shape["chan"]),
        mesh=mesh,
        in_specs=(
            P(None, "chan", "band", None),
            P(None, "chan", "band", None),
            P("chan", None),
            P("chan"),
            P("chan"),
            P(None, None, "chan", None),
            P("chan"),
            P("chan"),
            P("chan", None),
            P("chan"),
            P(),
        ),
        out_specs=P(None, None, ("band", "chan"), None),
        check_vma=False,
    )
```

```python
import functools
import math

import jax
import jax.numpy as jnp
from jax import lax
from jax.experimental import pallas as pl
from jax.experimental.pallas import tpu as pltpu
from jax.sharding import PartitionSpec as P

D = 256
GROUPS = 32
EPS = 1e-05
MESH = pl.DeviceIdType.MESH
F32 = jnp.float32
BF16 = jnp.bfloat16


def wait_on(ref, sem):
    pltpu.make_async_copy(ref, ref, sem).wait()


def kernel(
    bands, chans, pixel_count,
    fine, coarse, lat_in, par_in, conv_in, mask_in, queries,
    out,
    feats, level, ebuf, pbuf, wbuf, mbuf, wide, lat, cols_up, stacked, conv, rows_out, stat1, stat2,
    f_send, f_recv, fh_send, fh_recv, c_send, c_recv, ch_send, ch_recv,
    e_send, e_recv, w_send, w_recv, q_send, q_recv, s_send, s_recv, o_sem,
):
    images, band_rows, in_ch, width = fine.shape
    rows = band_rows // chans
    c_rows = coarse.shape[1] // chans
    c_ch = coarse.shape[2]
    share = lat_in.shape[1]
    quad = math.gcd(bands, 4)
    quarter = share // quad
    gsize = D // GROUPS
    total = bands * chans
    b = lax.axis_index("band")
    c = lax.axis_index("chan")
    me = b * chans + c
    sends = []

    def send(src, dst, ssem, rsem, tb, tc, maybe_self):
        def remote():
            return pltpu.make_async_remote_copy(
                src_ref=src, dst_ref=dst, send_sem=ssem, recv_sem=rsem,
                device_id=(tb, tc), device_id_type=MESH,
            )

        if not maybe_self:
            remote().start()
            sends.append((remote, None))
            return
        is_self = jnp.logical_and(tb == b, tc == c)

        @pl.when(is_self)
        def _():
            pltpu.make_async_copy(src, dst, rsem).start()

        @pl.when(jnp.logical_not(is_self))
        def _():
            remote().start()

        sends.append((remote, is_self))

    def block(index, size):
        return pl.ds(pl.multiple_of(index * size, size), size)

    def gather(src, dst, ssem, rsem):
        pltpu.make_async_copy(src, dst.at[c], rsem.at[0]).start()
        for s in range(1, chans):
            t = lax.rem(c + s, chans)
            send(src, dst.at[c], ssem.at[s], rsem.at[s], b, t, False)

    spot = lax.rem(b, quad)
    near_count = quad * chans

    def quarter_of(owner, part):
        return pl.ds(pl.multiple_of(owner * share + part * quarter, quarter), quarter)

    def weights_across(src, dst, ssem, rsem):
        pltpu.make_async_copy(src, dst.at[:, block(c, share)], rsem.at[0]).start()
        for s in range(1, chans):
            t = lax.rem(c + s, chans)
            send(
                src.at[:, pl.ds(pl.multiple_of(spot * quarter, quarter), quarter)],
                dst.at[:, quarter_of(c, spot)], ssem.at[s], rsem.at[s], b, t, False,
            )

    def weights_around(dst, rsem, ssem2, rsem2):
        for s in range(1, chans):
            wait_on(dst.at[:, pl.ds(0, quarter)], rsem.at[s])
            owner = lax.rem(c - s + chans, chans)
            piece = dst.at[:, quarter_of(owner, spot)]
            for m in range(1, quad):
                mate = b - spot + lax.rem(spot + m, quad)
                send(piece, piece, ssem2.at[s, m], rsem2.at[s, m], mate, c, False)

    def wait_weights(dst, rsem, rsem2):
        wait_on(dst.at[:, pl.ds(0, share)], rsem.at[0])
        for s in range(1, chans):
            for m in range(1, quad):
                wait_on(dst.at[:, pl.ds(0, quarter)], rsem2.at[s, m])

    def main_rows(src, dst, n, size, ch, ssem, rsem):
        for s in range(chans):
            t = lax.rem(c + s, chans)
            piece = src.at[n, pl.ds(t * size, size)]
            place = dst.at[n, pl.ds(1, size), block(c, ch)]
            if s == 0:
                pltpu.make_async_copy(piece, place, rsem.at[n, 0]).start()
            else:
                send(piece, place, ssem.at[n, s], rsem.at[n, s], b, t, False)

    def halo_rows(src, dst, n, size, ch, ssem, rsem):
        for s in range(chans):
            t = lax.rem(c + s, chans)
            k = (s + 1) % chans
            to = lax.rem(b * chans + t + 1, total)
            send(
                src.at[n, (t + 1) * size - 1], dst.at[n, 0, block(c, ch)],
                ssem.at[n, 0, s], rsem.at[n, 0, k], to // chans, lax.rem(to, chans), k == 0,
            )
            k = (s - 1) % chans
            to = lax.rem(b * chans + t - 1 + total, total)
            send(
                src.at[n, t * size], dst.at[n, size + 1, block(c, ch)],
                ssem.at[n, 1, s], rsem.at[n, 1, k], to // chans, lax.rem(to, chans), k == 0,
            )

    def wait_main(dst, n, size, ch, rsem):
        for s in range(chans):
            wait_on(dst.at[n, pl.ds(1, size), pl.ds(0, ch)], rsem.at[n, s])

    def wait_halo(dst, n, size, ch, rsem):
        for side in range(2):
            for s in range(chans):
                wait_on(dst.at[n, side * (size + 1), pl.ds(0, ch)], rsem.at[n, side, s])

    gather(lat_in, ebuf, e_send.at[0], e_recv.at[0])
    gather(par_in, pbuf, e_send.at[1], e_recv.at[1])
    for n in range(images):
        main_rows(fine, feats, n, rows, in_ch, f_send, f_recv)
    weights_across(conv_in, wbuf, w_send.at[0], w_recv.at[0])
    weights_across(mask_in, mbuf, w_send.at[1], w_recv.at[1])
    halo_rows(fine, feats, 0, rows, in_ch, fh_send, fh_recv)

    local_count = float(gsize * rows * width)
    lane = lax.broadcasted_iota(jnp.int32, (GROUPS, 128), 1)
    sub = lax.broadcasted_iota(jnp.int32, (GROUPS, 128), 0)

    def fold(x):
        acc = x[:, 0:128]
        for k in range(1, width // 128):
            acc = acc + x[:, k * 128:(k + 1) * 128]
        return acc

    def group_sum(x):
        x = jnp.sum(x.reshape(GROUPS, gsize, x.shape[1]), axis=1)
        return jnp.sum(x, axis=1, keepdims=True)

    def to_channels(col):
        return jnp.broadcast_to(col[:, None, :], (GROUPS, gsize, 1)).reshape(D, 1)

    def at_lanes(col, slot):
        return jnp.where(lane == sub + slot * GROUPS, jnp.broadcast_to(col, (GROUPS, 128)), 0.0)

    def from_lanes(row, slot):
        spread = jnp.where(lane == sub + slot * GROUPS, jnp.broadcast_to(row, (GROUPS, 128)), 0.0)
        return jnp.sum(spread, axis=1, keepdims=True)

    def produce(ref, n, first, compute):
        def step(r, acc):
            y = compute(r)
            ref[n, r + first] = y
            return acc + fold(y)

        s = group_sum(lax.fori_loop(0, rows, step, jnp.zeros((D, 128), F32)))
        mean = to_channels(s / local_count)

        def spread(r, acc):
            d = ref[n, r + first] - mean
            return acc + fold(d * d)

        m2 = group_sum(lax.fori_loop(0, rows, spread, jnp.zeros((D, 128), F32)))
        return at_lanes(s, n) + at_lanes(m2, images + n)

    def exchange(stats, buf, which):
        buf[0, 0] = jnp.sum(stats, axis=0, keepdims=True)

        def near_by(k, carry):
            to = lax.rem(spot * chans + c + k, near_count)
            pltpu.make_async_remote_copy(
                src_ref=buf.at[0, 0], dst_ref=buf.at[0, k],
                send_sem=s_send.at[which, 0], recv_sem=s_recv.at[which, 0],
                device_id=(b - spot + to // chans, lax.rem(to, chans)), device_id_type=MESH,
            ).start()
            return carry

        lax.fori_loop(1, near_count, near_by, 0)

    def spread_out(buf, which):
        wait_on(buf.at[0, pl.ds(1, near_count - 1)], s_recv.at[which, 0])

        def far_off(k, carry):
            pltpu.make_async_remote_copy(
                src_ref=buf.at[0], dst_ref=buf.at[k],
                send_sem=s_send.at[which, 1], recv_sem=s_recv.at[which, 1],
                device_id=(lax.rem(b + k * quad, bands), c), device_id_type=MESH,
            ).start()
            return carry

        lax.fori_loop(1, bands // quad, far_off, 0)

    def combined(buf, which):
        wait_on(buf.at[pl.ds(1, bands // quad - 1)], s_recv.at[which, 1])
        parts = buf[...].reshape(total, 1, 128)
        sums = jnp.sum(parts, axis=0)
        mean = sums / pixel_count
        off = parts / local_count - mean[None]
        m2 = pltpu.roll(sums, 128 - images * GROUPS, 1)
        var = (m2 + local_count * jnp.sum(off * off, axis=0)) / pixel_count
        inv = lax.rsqrt(var + EPS)
        return [
            (to_channels(from_lanes(mean, n)), to_channels(from_lanes(inv, n)))
            for n in range(images)
        ]

    for k in range(2):
        for s in range(chans):
            wait_on((ebuf, pbuf)[k].at[0], e_recv.at[k, s])
    square = (
        lax.broadcasted_iota(jnp.int32, (share, share), 0)
        == lax.broadcasted_iota(jnp.int32, (share, share), 1)
    )

    def column(k):
        return jnp.concatenate([
            jnp.sum(jnp.where(
                square, jnp.broadcast_to(pbuf[s].astype(F32)[k:k + 1], (share, share)), 0.0,
            ), axis=1, keepdims=True)
            for s in range(chans)
        ], axis=0)

    lat_gain, lat_shift, out_gain, out_shift, bias = (column(k) for k in range(5))

    def lateral(features):
        return jnp.concatenate([
            lax.dot_general(
                ebuf[s], features, (((0,), (0,)), ((), ())), preferred_element_type=F32)
            for s in range(chans)
        ], axis=0)

    stats = jnp.zeros((GROUPS, 128), F32)
    for n in range(images):
        wait_main(feats, n, rows, in_ch, f_recv)
        stats = stats + produce(lat, n, 1, lambda r, n=n: lateral(feats[n, r + 1]))
    exchange(stats, stat1, 0)
    for n in range(images):
        if n > 0:
            halo_rows(fine, feats, n, rows, in_ch, fh_send, fh_recv)
        main_rows(coarse, level, n, c_rows, c_ch, c_send, c_recv)
        halo_rows(coarse, level, n, c_rows, c_ch, ch_send, ch_recv)
    weights_around(wbuf, w_recv.at[0], q_send.at[0], q_recv.at[0])
    weights_around(mbuf, w_recv.at[1], q_send.at[1], q_recv.at[1])
    spread_out(stat1, 0)

    src_col = lax.broadcasted_iota(jnp.int32, (width // 2, width), 0)
    dst_col = lax.broadcasted_iota(jnp.int32, (width // 2, width), 1)
    half = dst_col // 2
    near = jnp.where(src_col == half, 0.75, 0.0)
    other = jnp.clip(jnp.where(dst_col - 2 * half == 0, half - 1, half + 1), 0, width // 2 - 1)
    up = (near + jnp.where(src_col == other, 0.25, 0.0)).astype(BF16)
    lane_w = lax.broadcasted_iota(jnp.int32, (D, width), 1)

    stats = jnp.zeros((GROUPS, 128), F32)
    norms = None
    for n in range(images):
        wait_halo(feats, n, rows, in_ch, fh_recv)
        for j in (0, rows + 1):
            lat[n, j] = lateral(feats[n, j])
        wait_main(level, n, c_rows, c_ch, c_recv)
        wait_halo(level, n, c_rows, c_ch, ch_recv)

        def widen(k, carry):
            cols_up[k] = jnp.dot(level[n, k], up, preferred_element_type=F32)
            return carry

        lax.fori_loop(0, c_rows + 2, widen, 0)

        @pl.when(me == 0)
        def _():
            cols_up[0] = cols_up[1]

        @pl.when(me == total - 1)
        def _():
            cols_up[c_rows + 1] = cols_up[c_rows]

        if norms is None:
            norms = combined(stat1, 0)
        mean, inv = norms[n]
        scale = inv * lat_gain

        def join(j, carry):
            k = j // 2
            even = j - 2 * k == 0
            w0 = jnp.where(even, 0.75, 0.25)
            w1 = jnp.where(even, 0.25, 0.75)
            upsampled = w0 * cols_up[k] + w1 * cols_up[k + 1]
            joined = (lat[n, j] - mean) * scale + lat_shift + upsampled
            inside = jnp.logical_and(me * rows + j >= 1, me * rows + j <= total * rows)
            joined = jnp.where(inside, joined, 0.0)
            left = jnp.where(lane_w == 0, 0.0, pltpu.roll(joined, 1, 1))
            right = jnp.where(lane_w == width - 1, 0.0, pltpu.roll(joined, width - 1, 1))
            base = pl.multiple_of(j * 3 * D, D)
            stacked[pl.ds(base, D)] = left.astype(BF16)
            stacked[pl.ds(base + D, D)] = joined.astype(BF16)
            stacked[pl.ds(base + 2 * D, D)] = right.astype(BF16)
            return carry

        lax.fori_loop(0, rows + 2, join, 0)
        if n == 0:
            wait_weights(wbuf, w_recv.at[0], q_recv.at[0])
            for k in range(9):
                wide[:, k * D:(k + 1) * D] = wbuf[k]

        def convolve(r):
            base = pl.multiple_of(r * 3 * D, D)
            return jnp.dot(wide[...], stacked[pl.ds(base, 9 * D)], preferred_element_type=F32)

        stats = stats + produce(conv, n, 0, convolve)

    exchange(stats, stat2, 1)
    spread_out(stat2, 1)
    wait_weights(mbuf, w_recv.at[1], q_recv.at[1])
    norms = combined(stat2, 1)
    for n in range(images):
        mean, inv = norms[n]
        scale = inv * out_gain

        def finish(r, carry):
            act = jnp.maximum((conv[n, r] - mean) * scale + out_shift, 0.0).astype(BF16)
            mixed = jnp.dot(mbuf[0], act, preferred_element_type=F32)
            features = (mixed + bias).astype(BF16)
            logits = jnp.dot(queries[...], features, preferred_element_type=F32)
            shifted = logits - jnp.max(logits, axis=0, keepdims=True)
            norm = jnp.log(jnp.sum(jnp.exp(shifted), axis=0, keepdims=True))
            rows_out[n, r] = shifted - norm
            pltpu.make_async_copy(rows_out.at[n, r], out.at[n, r], o_sem.at[n, r]).start()
            return carry

        lax.fori_loop(0, rows, finish, 0)

    for n in range(images):
        for r in range(rows):
            pltpu.make_async_copy(rows_out.at[n, r], out.at[n, r], o_sem.at[n, r]).wait()
    for which, buf in ((0, stat1), (1, stat2)):
        wait_on(buf.at[0, pl.ds(1, near_count - 1)], s_send.at[which, 0])
        wait_on(buf.at[pl.ds(1, bands // quad - 1)], s_send.at[which, 1])
    for remote, is_self in sends:
        if is_self is None:
            remote().wait_send()
        else:
            @pl.when(jnp.logical_not(is_self))
            def _():
                remote().wait_send()


def per_device(
    bands, chans,
    fine_features, coarse_level, lat_weight, lat_gain, lat_shift, out_weight, out_gain, out_shift,
    mask_weight, mask_bias, queries,
):
    images, in_ch, band_rows, width = fine_features.shape
    share = lat_weight.shape[0]
    c_ch, c_band = coarse_level.shape[1], coarse_level.shape[2]
    rows, c_rows = band_rows // chans, c_band // chans
    query_count = queries.shape[0]
    pixel_count = float(D // GROUPS * band_rows * bands * width)
    fine = jnp.transpose(fine_features, (0, 2, 1, 3))
    coarse = jnp.transpose(coarse_level, (0, 2, 1, 3))
    params = jnp.stack([lat_gain, lat_shift, out_gain, out_shift, mask_bias], axis=0)
    params = jnp.pad(params, ((0, 16 - params.shape[0]), (0, 0)))
    anywhere = pl.BlockSpec(memory_space=pl.ANY)
    vmem = pl.BlockSpec(memory_space=pltpu.VMEM)
    quad = math.gcd(bands, 4)
    dma = pltpu.SemaphoreType.DMA
    result = pl.pallas_call(
        functools.partial(kernel, bands, chans, pixel_count),
        out_shape=jax.ShapeDtypeStruct((images, rows, query_count, width), F32),
        in_specs=[anywhere] * 6 + [vmem],
        out_specs=anywhere,
        scratch_shapes=[
            pltpu.VMEM((images, rows + 2, chans * in_ch, width), BF16),
            pltpu.VMEM((images, c_rows + 2, chans * c_ch, width // 2), BF16),
            pltpu.VMEM((chans, chans * in_ch, share), BF16),
            pltpu.VMEM((chans, 16, share), BF16),
            pltpu.VMEM((9, D, D), BF16),
            pltpu.VMEM((1, D, D), BF16),
            pltpu.VMEM((D, 9 * D), BF16),
            pltpu.VMEM((images, rows + 2, D, width), F32),
            pltpu.VMEM((c_rows + 2, D, width), F32),
            pltpu.VMEM(((rows + 2) * 3 * D, width), BF16),
            pltpu.VMEM((images, rows, D, width), F32),
            pltpu.VMEM((images, rows, query_count, width), F32),
            pltpu.VMEM((bands // quad, quad * chans, 1, 128), F32),
            pltpu.VMEM((bands // quad, quad * chans, 1, 128), F32),
            dma((images, chans)), dma((images, chans)),
            dma((images, 2, chans)), dma((images, 2, chans)),
            dma((images, chans)), dma((images, chans)),
            dma((images, 2, chans)), dma((images, 2, chans)),
            dma((2, chans)), dma((2, chans)), dma((2, chans)), dma((2, chans)),
            dma((2, chans, 4)), dma((2, chans, 4)),
            dma((2, 2)), dma((2, 2)),
            dma((images, rows)),
        ],
        compiler_params=pltpu.CompilerParams(
            has_side_effects=True, vmem_limit_bytes=60 * 1024 * 1024),
    )(
        fine, coarse, lat_weight.T, params, out_weight.reshape(9, share, D), mask_weight[None],
        queries,
    )
    return jnp.transpose(result, (0, 2, 1, 3))


def solution(mesh):
    return jax.shard_map(
        functools.partial(per_device, mesh.shape["band"], mesh.shape["chan"]),
        mesh=mesh,
        in_specs=(
            P(None, "chan", "band", None),
            P(None, "chan", "band", None),
            P("chan", None),
            P("chan"),
            P("chan"),
            P(None, None, "chan", None),
            P("chan"),
            P("chan"),
            P("chan", None),
            P("chan"),
            P(),
        ),
        out_specs=P(None, None, ("band", "chan"), None),
        check_vma=False,
    )
```
